32 devices in a mesh: fsdp: 8 (over z, core), cols: 4 (over y, x).
Axes of the slice: x: 2, y: 2, z: 4, core: 2. Of those that a mesh axis runs over, the one named last changes fastest.
Arguments:
- one_query: float32 [4096, 4096], P('fsdp', 'cols'), may hold values from -0.125 to 0.125
- other_query: float32 [4096, 4096], P('fsdp', 'cols'), may hold values from -0.09375 to 0.09375
- one_key: float32 [4096, 4096], P('fsdp', 'cols'), may hold values from -0.125 to 0.125
- other_key: float32 [4096, 4096], P('fsdp', 'cols'), may hold values from -0.09375 to 0.09375
- one_value: float32 [4096, 4096], P('fsdp', 'cols'), may hold values from -0.125 to 0.125
- other_value: float32 [4096, 4096], P('fsdp', 'cols'), may hold values from -0.09375 to 0.09375
- mix_share: float32 [4096], P('fsdp'), may hold values from 0.2 to 0.8
- norm_train: float32 [4096], P(('fsdp', 'cols')), may hold values from 0.25 to 1.75
- norm_step: float32 [4096], P(('fsdp', 'cols')), may hold values from -0.3 to 0.3
Outputs:
- final_query: bfloat16 [4096, 4096], P(None, 'cols')
- final_key: bfloat16 [4096, 4096], P(None, 'cols')
- final_value: bfloat16 [4096, 4096], P(None, 'cols')
- scale_query: float32 [4096], P('cols')
- scale_key: float32 [4096], P('cols')
- scale_value: float32 [4096], P('cols')
- serve_norm: bfloat16 [4096], replicated
The draws below stay inside these ranges and needn't reach their ends.
All inputs are finite; a program needn't handle non-finite values.
Results may differ from the reference program's by a relative error of at most 0.0004.
Values may be sent and summed in bfloat16 or wider, within the bound.
A program may use at most 128 MiB of HBM per device.

```python
import jax
import jax.numpy as jnp
from jax import lax

D_MODEL = 4096
Q_DIM = 4096
KV_DIM = 4096


def with_spikes(values, stream_key, source, target, shards_of, factor):
    owner, partner = [(jnp.arange(values.shape[position]) // (values.shape[position] // shards_of)).reshape([-1 if axis == position else 1 for axis in range(values.ndim)]) for position in (source, target)]
    chosen = jax.random.permutation(stream_key, shards_of)[partner]
    strong = (owner == chosen) | (owner == (partner + shards_of // 2) % shards_of)
    return jnp.where(strong, factor * values, values)


def level_of(rng, extent, split, low, top_value):
    loudness = 1.0
    for position, parts in split:
        steps = jax.random.uniform(jax.random.fold_in(jax.random.fold_in(rng, 6), position), (parts,), jnp.float32, low / len(split), top_value / len(split))
        loudness = loudness * jnp.repeat(jnp.exp(steps), extent[position] // parts).reshape((-1,) + (1,) * (len(extent) - 1 - position))
    return loudness


def noise(stream_key, dims, deviation, limit, shards=(), held_as=jnp.bfloat16):
    factor_of = level_of(stream_key, dims, shards, -0.22, 0.18) if shards else 1.0
    drawn = jax.random.normal(stream_key, dims, jnp.float32) * deviation * factor_of
    return jnp.minimum(jnp.maximum(drawn, -limit), limit).astype(held_as)


def gaussian_with(stream_key, dims, scale, most, cuts, heavy, dtype=jnp.bfloat16):
    values = scale * jax.random.normal(stream_key, dims, jnp.float32)
    if cuts:
        values = values * level_of(stream_key, dims, cuts, -0.22, 0.18)
    return jnp.clip(with_spikes(values, jax.random.fold_in(stream_key, 3), *heavy), -most, most).astype(dtype)


def setup_inputs(seed: int = 0) -> dict:
    key_list = jax.random.split(jax.random.key(seed), 10)
    one_query = gaussian_with(key_list[0], (D_MODEL, Q_DIM), D_MODEL ** -0.5, 0.125, ((0, 8), (1, 4)), (0, 1, 8, 2.0), jnp.float32)
    other_query = noise(key_list[1], (D_MODEL, Q_DIM), D_MODEL ** -0.5, 0.09375, ((0, 8), (1, 4)), jnp.float32)
    one_key = gaussian_with(key_list[2], (D_MODEL, KV_DIM), D_MODEL ** -0.5, 0.125, ((0, 8), (1, 4)), (0, 1, 8, 2.0), jnp.float32)
    other_key = noise(key_list[3], (D_MODEL, KV_DIM), D_MODEL ** -0.5, 0.09375, ((0, 8), (1, 4)), jnp.float32)
    one_value = gaussian_with(key_list[4], (D_MODEL, KV_DIM), D_MODEL ** -0.5, 0.125, ((0, 8), (1, 4)), (0, 1, 8, 2.0), jnp.float32)
    other_value = noise(key_list[5], (D_MODEL, KV_DIM), D_MODEL ** -0.5, 0.09375, ((0, 8), (1, 4)), jnp.float32)
    mix_share = jnp.clip(0.2 + 0.6 * jax.random.uniform(key_list[6], (D_MODEL,), jnp.float32) ** level_of(key_list[6], (D_MODEL,), ((0, 8),), -0.2, 0.2), 0.2, 0.8)
    norm_train = jnp.clip(1.0 + 0.15 * jax.random.normal(key_list[7], (D_MODEL,), jnp.float32), 0.25, 1.75)
    norm_step = jnp.clip(jax.random.uniform(key_list[8], (D_MODEL,), jnp.float32, -0.3, 0.3) * level_of(key_list[8], (D_MODEL,), ((0, 32),), -0.4, 0.0), -0.3, 0.3)
    return dict(one_query=one_query, other_query=other_query, one_key=one_key, other_key=other_key, one_value=one_value, other_value=other_value, mix_share=mix_share, norm_train=norm_train, norm_step=norm_step)


def reference(one_query, other_query, one_key, other_key, one_value, other_value, mix_share, norm_train, norm_step):
    result_query = mix_share[:, None] * one_query + (1.0 - mix_share[:, None]) * other_query
    result_key = mix_share[:, None] * one_key + (1.0 - mix_share[:, None]) * other_key
    result_value = mix_share[:, None] * one_value + (1.0 - mix_share[:, None]) * other_value
    scale_query = jnp.sqrt(lax.optimization_barrier(jnp.sum(result_query * result_query, axis=0)))
    final_query = (result_query / scale_query).astype(jnp.bfloat16)
    scale_key = jnp.sqrt(lax.optimization_barrier(jnp.sum(result_key * result_key, axis=0)))
    final_key = (result_key / scale_key).astype(jnp.bfloat16)
    scale_value = jnp.sqrt(lax.optimization_barrier(jnp.sum(result_value * result_value, axis=0)))
    final_value = (result_value / scale_value).astype(jnp.bfloat16)
    serve_norm = (norm_train + norm_step).astype(jnp.bfloat16)
    return (final_query, final_key, final_value, scale_query, scale_key, scale_value, serve_norm)
```

```python
import functools

import jax
import jax.numpy as jnp
from jax import lax
from jax.experimental import pallas as pl
from jax.experimental.pallas import tpu as pltpu
from jax.sharding import PartitionSpec as P

MESH = pl.DeviceIdType.MESH
LANES = 128
PIECES = ((0, 0, 1), (0, 1, 1), (0, 2, 6), (1, 0, 8), (2, 0, 6), (2, 6, 2))
LOADS = 4
HELD_OWN = 8
HELD_NEXT = 2
HELD = HELD_OWN + HELD_NEXT
CHUNKS = ((2, 6, 2, 8), (1, 0, 4, 0), (1, 4, 2, 4), (1, 6, 1, 6), (1, 7, 1, 7))


def gather_kernel(F, C, *refs):
    ins, mix_ref, train_ref, step_ref = refs[0:6], refs[6], refs[7], refs[8]
    outs, scale_out, norm_out = refs[9:12], refs[12], refs[13]
    (held, mixb, sums, in_sem, sum_send, sum_recv, norm_sem, up_send, down_send,
     pair_send, line_recv, pair_recv, early, early_send, early_recv) = refs[14:]
    rows, width = ins[0].shape
    Z = F // 2
    me = lax.axis_index("fsdp")
    col = lax.axis_index("cols")
    z = me // 2
    core = lax.rem(me, 2)
    eighth = rows // 8
    K = len(PIECES)

    def at(f):
        return {"fsdp": f}

    load_rows = rows // LOADS

    def load(i, p):
        r = pl.ds(p * load_rows, load_rows)
        return pltpu.make_async_copy(ins[i].at[r, :], held.at[i, r, :], in_sem.at[i, p])

    for p in range(LOADS):
        load(0, p).start()
        load(1, p).start()

    barrier = pltpu.get_barrier_semaphore()
    for d in range(1, F):
        pl.semaphore_signal(barrier, inc=1, device_id=(lax.rem(me + d, F), col), device_id_type=MESH)
    for d in range(1, C):
        pl.semaphore_signal(barrier, inc=1, device_id=(me, lax.rem(col + d, C)), device_id_type=MESH)

    for g in range(rows // LANES):
        row = mix_ref[pl.ds(g, 1), :]
        mixb[pl.ds(g * LANES, LANES), :] = jnp.broadcast_to(row, (LANES, LANES)).T
    norm_out[me, col] = train_ref[...] + step_ref[...]

    def mix(a):
        def body(i, acc):
            r = pl.ds(pl.multiple_of(i * 8, 8), 8)
            m = mixb[r, :]
            n = 1.0 - m
            new = []
            for j in range(width // LANES):
                c = pl.ds(j * LANES, LANES)
                v = m * held[2 * a, r, c] + n * held[2 * a + 1, r, c]
                held[2 * a, r, c] = v
                new.append(acc[j] + v * v)
            return tuple(new)

        zero = jnp.zeros((8, LANES), jnp.float32)
        acc = (zero,) * (width // LANES)
        for p in range(LOADS):
            load(2 * a, p).wait()
            load(2 * a + 1, p).wait()
            acc = lax.fori_loop(p * load_rows // 8, (p + 1) * load_rows // 8, body, acc, unroll=2)
            if a == 0 and p == LOADS - 2:
                for i in range(2, 6):
                    for later in range(LOADS):
                        load(i, later).start()
        for j in range(width // LANES):
            sums[a, me, :, pl.ds(j * LANES, LANES)] = jnp.sum(acc[j], axis=0, keepdims=True)

    def sum_copy(a, d):
        peer = lax.rem(me + d, F)
        return pltpu.make_async_remote_copy(
            src_ref=sums.at[a, me], dst_ref=sums.at[a, me],
            send_sem=sum_send.at[a], recv_sem=sum_recv.at[a],
            device_id=(peer, col), device_id_type=MESH)

    def all_sums(a):
        ref = sums.at[a, pl.ds(0, F - 1)]
        return pltpu.make_async_remote_copy(
            src_ref=ref, dst_ref=ref, send_sem=sum_send.at[a], recv_sem=sum_recv.at[a],
            device_id=(lax.rem(me + 1, F), col), device_id_type=MESH)

    def norm_copy1(d):
        return pltpu.make_async_remote_copy(
            src_ref=norm_out.at[me, col], dst_ref=norm_out.at[me, col],
            send_sem=norm_sem.at[0], recv_sem=norm_sem.at[1],
            device_id=(me, lax.rem(col + d, C)), device_id_type=MESH)

    def norm_copy2(d):
        return pltpu.make_async_remote_copy(
            src_ref=norm_out.at[me], dst_ref=norm_out.at[me],
            send_sem=norm_sem.at[2], recv_sem=norm_sem.at[3],
            device_id=(lax.rem(me + d, F), col), device_id_type=MESH)

    def all_norm1():
        ref = norm_out.at[me, pl.ds(0, C - 1)]
        return pltpu.make_async_remote_copy(
            src_ref=ref, dst_ref=ref, send_sem=norm_sem.at[0], recv_sem=norm_sem.at[1],
            device_id=(me, lax.rem(col + 1, C)), device_id_type=MESH)

    def all_norm2():
        ref = norm_out.at[pl.ds(0, F - 1)]
        return pltpu.make_async_remote_copy(
            src_ref=ref, dst_ref=ref, send_sem=norm_sem.at[2], recv_sem=norm_sem.at[3],
            device_id=(lax.rem(me + 1, F), col), device_id_type=MESH)

    mix(0)
    pl.semaphore_wait(barrier, F - 1 + C - 1)
    for d in range(1, F):
        sum_copy(0, d).start()
    early_rows = pl.ds(0, eighth)
    early_down = pltpu.make_async_remote_copy(
        src_ref=held.at[0, early_rows, :], dst_ref=early, send_sem=early_send.at[0],
        recv_sem=early_recv, device_id=(me - 2, col), device_id_type=MESH)
    early_up = pltpu.make_async_remote_copy(
        src_ref=held.at[0, early_rows, :], dst_ref=early, send_sem=early_send.at[1],
        recv_sem=early_recv, device_id=(me + 2, col), device_id_type=MESH)

    @pl.when(z == 1)
    def _():
        early_down.start()

    @pl.when(z == Z - 2)
    def _():
        early_up.start()

    for d in range(1, C):
        norm_copy1(d).start()
    mix(1)
    for d in range(1, F):
        sum_copy(1, d).start()
    mix(2)
    for d in range(1, F):
        sum_copy(2, d).start()

    def send(k, source, target, sender, receiver):
        a, first, count = PIECES[k]
        start = pl.multiple_of(source * rows + first * eighth, eighth)
        ref = outs[a].at[pl.ds(start, count * eighth), :]
        return pltpu.make_async_remote_copy(
            src_ref=ref, dst_ref=ref, send_sem=sender, recv_sem=receiver,
            device_id=(target, col), device_id_type=MESH)

    def up(k, s):
        a = PIECES[k][0]
        return send(k, 2 * s + core, me + 2, up_send.at[a], line_recv.at[s * K + k])

    def down(k, s):
        a = PIECES[k][0]
        return send(k, 2 * s + core, me - 2, down_send.at[a], line_recv.at[s * K + k])

    def pair(k, s):
        a = PIECES[k][0]
        return send(k, 2 * s + core, 2 * z + 1 - core, pair_send.at[a], pair_recv.at[a])

    def span(a, count, sender, receiver):
        ref = outs[a].at[pl.ds(0, count), :]
        return pltpu.make_async_remote_copy(
            src_ref=ref, dst_ref=ref, send_sem=sender.at[a], recv_sem=receiver.at[a],
            device_id=(2 * z + 1 - core, col), device_id_type=MESH)

    def held_piece(k, d):
        return jnp.logical_or(d == 1, d == 2) if k == K - 1 else d == 1

    def goes_down(k, s):
        if k == 0:
            return jnp.logical_and(z > 0, jnp.logical_or(z != 1, s != z))
        if PIECES[k][0] == 2:
            return jnp.logical_and(z > 0, jnp.logical_not(jnp.logical_and(z == 1, held_piece(k, s))))
        return z > 0

    def goes_up(k, s):
        if k == 0:
            return jnp.logical_and(z < Z - 1, jnp.logical_or(z != Z - 2, s != z))
        if PIECES[k][0] == 2:
            return jnp.logical_and(
                z < Z - 1, jnp.logical_not(jnp.logical_and(z == Z - 2, held_piece(k, Z - 1 - s))))
        return z < Z - 1

    def comes(k, hop, there, end):
        if PIECES[k][0] == 2:
            return jnp.logical_and(there, jnp.logical_not(jnp.logical_and(end, held_piece(k, hop))))
        return there

    def start_own(k):
        @pl.when(goes_down(k, z))
        def _():
            down(k, z).start()

        @pl.when(goes_up(k, z))
        def _():
            up(k, z).start()

        pair(k, z).start()

    def normalize(a, source, target, count, inverse):
        def body(i, carry):
            r = pl.ds(pl.multiple_of(i * 16, 16), 16)
            o = pl.ds(pl.multiple_of(target + i * 16, 16), 16)
            outs[a][o, :] = (source[r, :] * inverse).astype(jnp.bfloat16)
            return carry

        lax.fori_loop(0, count // 16, body, 0, unroll=2)

    inverses = []
    for k, (a, first, count) in enumerate(PIECES):
        if len(inverses) == a:
            all_sums(a).wait_recv()
            total = sums[a, 0]
            for f in range(1, F):
                total = total + sums[a, f]
            scale = jnp.sqrt(total)
            scale_out[a] = scale
            inverses.append(1.0 / scale)
        inverse = jnp.broadcast_to(inverses[a], (16, width))
        size = count * eighth
        normalize(a, held.at[2 * a, pl.ds(first * eighth, size), :],
                  me * rows + first * eighth, size, inverse)
        if k > 0:
            start_own(k - 1)
    all_norm1().wait_recv()
    for d in range(1, F):
        norm_copy2(d).start()
    start_own(K - 1)

    def take_early(owner):
        early_down.wait_recv()
        inverse = jnp.broadcast_to(1.0 / scale_out[0], (16, width))
        normalize(0, early, (2 * owner + core) * rows, eighth, inverse)

    def relay(hop, carry):
        for k in range(K):
            @pl.when(comes(k, hop, z + hop < Z, z == 0))
            def _(k=k):
                if k == 0:
                    is_early = jnp.logical_and(z == 0, hop == 1)

                    @pl.when(is_early)
                    def _():
                        take_early(1)

                    @pl.when(jnp.logical_not(is_early))
                    def _():
                        down(k, z + hop).wait_recv()
                else:
                    down(k, z + hop).wait_recv()

                @pl.when(goes_down(k, z + hop))
                def _():
                    down(k, z + hop).start()

                pair(k, z + hop).start()

            @pl.when(comes(k, hop, z - hop >= 0, z == Z - 1))
            def _(k=k):
                if k == 0:
                    is_early = jnp.logical_and(z == Z - 1, hop == 1)

                    @pl.when(is_early)
                    def _():
                        take_early(Z - 2)

                    @pl.when(jnp.logical_not(is_early))
                    def _():
                        up(k, z - hop).wait_recv()
                else:
                    up(k, z - hop).wait_recv()

                @pl.when(goes_up(k, z - hop))
                def _():
                    up(k, z - hop).start()

                pair(k, z - hop).start()

        return carry

    lax.fori_loop(1, Z, relay, 0)

    late = [(K - 1, 2)] + [(k, 1) for k in range(K) if PIECES[k][0] == 2]

    @pl.when(jnp.logical_and(core == 1, z == 1))
    def _():
        for k, d in late:
            down(k, d).start()

    @pl.when(jnp.logical_and(core == 1, z == Z - 2))
    def _():
        for k, d in late:
            up(k, Z - 1 - d).start()

    @pl.when(z == 1)
    def _():
        early_down.wait_send()

    @pl.when(z == Z - 2)
    def _():
        early_up.wait_send()

    for a in range(3):
        all_sums(a).wait_send()
    all_norm1().wait_send()
    all_norm2().wait_send()
    all_norm2().wait_recv()
    absent = HELD * eighth
    is_end = jnp.logical_or(z == 0, z == Z - 1)
    for a in range(2):
        span(a, Z * rows, pair_send, pair_recv).wait_send()
        span(a, Z * rows, pair_send, pair_recv).wait_recv()

    @pl.when(is_end)
    def _():
        span(2, Z * rows - absent, pair_send, pair_recv).wait_send()
        span(2, Z * rows - absent, pair_send, pair_recv).wait_recv()

    @pl.when(jnp.logical_not(is_end))
    def _():
        span(2, Z * rows, pair_send, pair_recv).wait_send()
        span(2, Z * rows, pair_send, pair_recv).wait_recv()

    def sent(a, count, less, toward, sender):
        if a == 0:
            count -= eighth if toward else 0
        if a < 2 or not toward:
            span(a, count, sender, pair_recv).wait_send()
            return

        @pl.when(core == 0)
        def _():
            span(a, count - less, sender, pair_recv).wait_send()

        @pl.when(core == 1)
        def _():
            span(a, count, sender, pair_recv).wait_send()

    for place in range(Z):
        @pl.when(z == place)
        def _(place=place):
            for a in range(3):
                if place > 0:
                    sent(a, (Z - place) * rows, absent, place == 1, down_send)
                if place < Z - 1:
                    sent(a, (place + 1) * rows, absent, place == Z - 2, up_send)

    @pl.when(jnp.logical_and(core == 1, z == 0))
    def _():
        for k, d in late:
            down(k, d).wait_recv()

    @pl.when(jnp.logical_and(core == 1, z == Z - 1))
    def _():
        for k, d in late:
            up(k, Z - 1 - d).wait_recv()


def place_of(F):
    me = lax.axis_index("fsdp")
    z, core, Z = me // 2, lax.rem(me, 2), F // 2
    return me, z, core, Z, jnp.logical_or(z == 0, z == Z - 1)


def store_kernel(F, pieces, *refs):
    gathered, scales, norm = refs[0:3], refs[3], refs[4]
    finals, scale_outs, norm_out, token = refs[5:8], refs[8:11], refs[11], refs[12]
    flat, flat_norm, flat_scales, sem, small_sem = refs[13:]
    me, z, core, Z, is_end = place_of(F)
    near = jnp.where(z == 0, 1, Z - 2)
    width = gathered[0].shape[1]
    rows = gathered[0].shape[0] // F
    part = F * rows // pieces
    copies = []
    for a in range(2):
        for p in range(pieces):
            r = pl.ds(p * part, part)
            copies.append(pltpu.make_async_copy(
                gathered[a].at[r, :], finals[a].at[r, :], sem.at[a * pieces + p]))
    for copy in copies:
        copy.start()
    blocks = []
    for f in range(F):
        r = pl.ds(f * rows, rows)
        absent = jnp.logical_and(is_end, near == f // 2)
        if f % 2:
            absent = jnp.logical_and(absent, core == 0)
        blocks.append((jnp.logical_not(absent), pltpu.make_async_copy(
            gathered[2].at[r, :], finals[2].at[r, :], sem.at[2 * pieces + f])))
    for there, copy in blocks:
        @pl.when(there)
        def _(copy=copy):
            copy.start()
    for a in range(3):
        for j in range(width // LANES):
            flat_scales[a, pl.ds(j, 1), :] = scales[a, :, pl.ds(j * LANES, LANES)]
    C = norm.shape[1]
    for f in range(F):
        for c in range(C):
            flat[pl.ds(f * C + c, 1), :] = norm[f, c]
    flat_norm[...] = flat[...].astype(jnp.bfloat16)
    small = [pltpu.make_async_copy(flat_scales.at[a], scale_outs[a], small_sem.at[a]) for a in range(3)]
    small.append(pltpu.make_async_copy(flat_norm, norm_out, small_sem.at[3]))
    for copy in small:
        copy.start()
    token[...] = jnp.zeros_like(token)
    for copy in copies + small:
        copy.wait()
    for there, copy in blocks:
        @pl.when(there)
        def _(copy=copy):
            copy.wait()


def held_kernel(F, value, token, y, line_send, line_recv, pair_sem, cross_sem):
    del token
    me, z, core, Z, is_end = place_of(F)
    col = lax.axis_index("cols")
    rows = value.shape[0] // F
    eighth = rows // 8
    low = z <= 1
    inward = jnp.where(low, me + 2, me - 2)
    outward = jnp.where(low, me - 2, me + 2)
    partner = 2 * z + 1 - core
    at_near = jnp.logical_and(core == 0, jnp.logical_or(z == 1, z == Z - 2))
    end0 = jnp.logical_and(is_end, core == 0)
    end1 = jnp.logical_and(is_end, core == 1)

    def block(d, parity, first, count):
        s = jnp.where(low, d, Z - 1 - d)
        start = pl.multiple_of((2 * s + parity) * rows + first * eighth, eighth)
        return value.at[pl.ds(start, count * eighth), :]

    def line(i):
        d, first, count, at = CHUNKS[i]
        return pltpu.make_async_remote_copy(
            src_ref=block(d, 0, first, count), dst_ref=y.at[0, pl.ds(at * eighth, count * eighth), :],
            send_sem=line_send, recv_sem=line_recv.at[i], device_id=(outward, col), device_id_type=MESH)

    def hand(i):
        d, first, count, at = CHUNKS[i]
        ref = y.at[0, pl.ds(at * eighth, count * eighth), :]
        return pltpu.make_async_remote_copy(
            src_ref=ref, dst_ref=ref, send_sem=pair_sem.at[0], recv_sem=pair_sem.at[1],
            device_id=(partner, col), device_id_type=MESH)

    def cross(d, first, count, at):
        return pltpu.make_async_remote_copy(
            src_ref=block(d, 1, first, count), dst_ref=y.at[1, pl.ds(at * eighth, count * eighth), :],
            send_sem=cross_sem.at[0], recv_sem=cross_sem.at[1], device_id=(partner, col), device_id_type=MESH)

    def whole(sender, receiver):
        ref = y.at[0]
        return pltpu.make_async_remote_copy(
            src_ref=ref, dst_ref=ref, send_sem=sender, recv_sem=receiver,
            device_id=(partner, col), device_id_type=MESH)

    barrier = pltpu.get_barrier_semaphore()

    @pl.when(end0)
    def _():
        pl.semaphore_signal(barrier, inc=1, device_id=(inward, col), device_id_type=MESH)

    @pl.when(is_end)
    def _():
        pl.semaphore_signal(barrier, inc=1, device_id=(partner, col), device_id_type=MESH)

    @pl.when(jnp.logical_or(at_near, is_end))
    def _():
        pl.semaphore_wait(barrier, 1)

    @pl.when(at_near)
    def _():
        for i in range(len(CHUNKS)):
            line(i).start()
        whole(line_send, pair_sem.at[1]).wait_send()

    @pl.when(end1)
    def _():
        cross(1, 0, HELD_OWN, 0).start()
        cross(2, 8 - HELD_NEXT, HELD_NEXT, HELD_OWN).start()
        whole(cross_sem.at[0], cross_sem.at[1]).wait_send()
        whole(pair_sem.at[0], pair_sem.at[1]).wait_recv()

    @pl.when(end0)
    def _():
        for i in range(len(CHUNKS)):
            line(i).wait_recv()
            hand(i).start()
        whole(cross_sem.at[0], cross_sem.at[1]).wait_recv()
        whole(pair_sem.at[0], pair_sem.at[1]).wait_send()


def patch_kernel(F, stored, y, out, sem):
    del stored
    me, z, core, Z, is_end = place_of(F)
    rows = out.shape[0] // F
    eighth = rows // 8
    low = z <= 1

    def patch(parity):
        copies = []
        for n, (d, first, count, at) in enumerate(((1, 0, HELD_OWN, 0), (2, 8 - HELD_NEXT, HELD_NEXT, HELD_OWN))):
            s = jnp.where(low, d, Z - 1 - d)
            start = pl.multiple_of((2 * s + parity) * rows + first * eighth, eighth)
            copies.append(pltpu.make_async_copy(
                y.at[parity, pl.ds(at * eighth, count * eighth), :],
                out.at[pl.ds(start, count * eighth), :], sem.at[2 * parity + n]))
        return copies

    both = jnp.logical_and(is_end, core == 0)

    @pl.when(is_end)
    def _():
        for copy in patch(0):
            copy.start()

    @pl.when(both)
    def _():
        for copy in patch(1):
            copy.start()
        for copy in patch(1):
            copy.wait()

    @pl.when(is_end)
    def _():
        for copy in patch(0):
            copy.wait()


def per_device(F, C, one_query, other_query, one_key, other_key, one_value, other_value,
               mix_share, norm_train, norm_step):
    rows, width = one_query.shape
    count = norm_train.shape[0]
    Z = F // 2
    K = len(PIECES)
    whole = (F * rows, width)
    any_spec = pl.BlockSpec(memory_space=pl.ANY)
    vmem = pl.BlockSpec(memory_space=pltpu.VMEM)
    dma = pltpu.SemaphoreType.DMA
    sent = 3 * rows * width * 2 * Z
    gathered = pl.pallas_call(
        functools.partial(gather_kernel, F, C), name="gather",
        out_shape=[pltpu.VMEM(whole, jnp.bfloat16)] * 3 + [
            pltpu.VMEM((3, 1, width), jnp.float32),
            pltpu.VMEM((F, C, 1, count), jnp.float32),
        ],
        in_specs=[pl.BlockSpec(memory_space=pltpu.HBM)] * 6 + [vmem] * 3,
        out_specs=[vmem] * 5,
        scratch_shapes=[
            pltpu.VMEM((6, rows, width), jnp.float32),
            pltpu.VMEM((rows, LANES), jnp.float32),
            pltpu.VMEM((3, F, 1, width), jnp.float32),
            dma((6, LOADS)),
            dma((3,)), dma((3,)), dma((4,)),
            dma((3,)), dma((3,)), dma((3,)), dma((Z * K,)), dma((3,)),
            pltpu.VMEM((rows // 8, width), jnp.float32), dma((2,)), dma,
        ],
        compiler_params=pltpu.CompilerParams(
            collective_id=0, has_side_effects=True, vmem_limit_bytes=VLIM),
        cost_estimate=pl.CostEstimate(flops=0, bytes_accessed=sent, transcendentals=0),
    )(one_query, other_query, one_key, other_key, one_value, other_value,
      mix_share.reshape(rows // LANES, LANES), norm_train.reshape(1, count),
      norm_step.reshape(1, count))
    pieces = 4
    hbm = pl.BlockSpec(memory_space=pltpu.HBM)
    finals = pl.pallas_call(
        functools.partial(store_kernel, F, pieces), name="store",
        out_shape=[pltpu.HBM(whole, jnp.bfloat16)] * 3
        + [jax.ShapeDtypeStruct((width // LANES, LANES), jnp.float32)] * 3
        + [jax.ShapeDtypeStruct((F * C, count), jnp.bfloat16), pltpu.VMEM((8, LANES), jnp.float32)],
        in_specs=[vmem] * 5,
        out_specs=[hbm] * 3 + [any_spec] * 4 + [vmem],
        scratch_shapes=[
            pltpu.VMEM((F * C, count), jnp.float32), pltpu.VMEM((F * C, count), jnp.bfloat16),
            pltpu.VMEM((3, width // LANES, LANES), jnp.float32), dma((2 * pieces + F,)), dma((4,)),
        ],
        compiler_params=pltpu.CompilerParams(vmem_limit_bytes=VLIM2),
    )(*gathered)
    eighth = rows // 8
    y = pl.pallas_call(
        functools.partial(held_kernel, F), name="held",
        out_shape=pltpu.VMEM((2, HELD * eighth, width), jnp.bfloat16),
        in_specs=[vmem, vmem], out_specs=vmem,
        scratch_shapes=[dma, dma((len(CHUNKS),)), dma((2,)), dma((2,))],
        compiler_params=pltpu.CompilerParams(
            collective_id=1, has_side_effects=True, vmem_limit_bytes=VLIM2),
        cost_estimate=pl.CostEstimate(flops=0, bytes_accessed=HELD * eighth * width * 2, transcendentals=0),
    )(gathered[2], finals[7])
    value = pl.pallas_call(
        functools.partial(patch_kernel, F), name="patch",
        out_shape=pltpu.HBM(whole, jnp.bfloat16),
        in_specs=[hbm, vmem], out_specs=hbm, input_output_aliases={0: 0},
        scratch_shapes=[dma((4,))],
        compiler_params=pltpu.CompilerParams(vmem_limit_bytes=VLIM2),
    )(finals[2], y)
    return (finals[0], finals[1], value, *(s.reshape(width) for s in finals[3:6]),
            finals[6].reshape(F * C * count))


VLIM = 36 * 1024 * 1024
VLIM2 = 2 * 1024 * 1024


def solution(mesh):
    F, C = mesh.shape["fsdp"], mesh.shape["cols"]
    block, fsdp, both = P("fsdp", "cols"), P("fsdp"), P(("fsdp", "cols"))
    return jax.shard_map(
        functools.partial(per_device, F, C), mesh=mesh,
        in_specs=(block,) * 6 + (fsdp, both, both),
        out_specs=(P(None, "cols"),) * 3 + (P("cols"),) * 3 + (P(),),
        check_vma=False)
```
